32 devices in a mesh: rows: 4 (over y, core), cols: 8 (over z, x).
Axes of the slice: x: 2, y: 2, z: 4, core: 2. Of those that a mesh axis runs over, the one named last changes fastest.
Arguments:
- tracer: float32 [384, 256, 128], P('rows', 'cols'), may hold values from 0.2 to 1.8
- crowding: float32 [384, 256, 128], P('rows', 'cols'), may hold values from 0.5 to 2
Outputs:
- potential: float32 [384, 256, 128], P('rows', 'cols')
- tracer_end: float32 [384, 256, 128], P('rows', 'cols')
The draws below stay inside these ranges and needn't reach their ends.
All inputs are finite; a program needn't handle non-finite values.
Results may differ from the reference program's by a relative error of at most 0.00002.
Values sent between devices are 32-bit elements; how exact they have to be, the bound alone decides.
A program may use at most 64 MiB of HBM per device.

```python
import jax
import jax.numpy as jnp
from jax import lax

GRID_Y = 384
GRID_X = 256
MEMBERS = 128
STEPS = 6


def block_levels(stream_key, extent, pieces, smallest, largest):
    def one(dim, parts):
        draws = jax.random.uniform(jax.random.fold_in(jax.random.fold_in(stream_key, 6), dim), (parts,), jnp.float32, smallest / len(pieces), largest / len(pieces))
        return jnp.repeat(jnp.exp(draws), extent[dim] // parts).reshape((-1,) + (1,) * (len(extent) - dim - 1))

    loudness = one(*pieces[0])
    for cut in pieces[1:]:
        loudness = loudness * one(*cut)
    return loudness


def setup_inputs(seed: int = 0) -> dict:
    streams_of = jax.random.split(jax.random.key(seed), 3)
    tracer = jnp.clip(0.2 + 1.5999999 * jax.random.uniform(streams_of[0], (GRID_Y, GRID_X, MEMBERS), jnp.float32) ** block_levels(streams_of[0], (GRID_Y, GRID_X, MEMBERS), ((0, 4), (1, 8)), -0.2, 0.2), 0.2, 1.8)
    crowding = jnp.clip(0.5 + 1.5 * jax.random.uniform(streams_of[1], (GRID_Y, GRID_X, MEMBERS), jnp.float32) ** block_levels(streams_of[1], (GRID_Y, GRID_X, MEMBERS), ((0, 4), (1, 8)), -0.2, 0.2), 0.5, 2.0)
    return dict(tracer=tracer, crowding=crowding)


def strip_edges(values, dims):
    for dim in dims:
        values = lax.slice_in_dim(values, 1, values.shape[dim] - 1, axis=dim)
    return values


def neighbour(values, dim, start, dims):
    others = [other for other in dims if other != dim]
    values = strip_edges(values, others)
    return lax.slice_in_dim(values, start, start + values.shape[dim] - 2, axis=dim)


def one_step(padded, crowding):
    middle = strip_edges(padded, (0, 1))
    lower = [neighbour(padded, dim, 0, (0, 1)) for dim in (0, 1)]
    upper = [neighbour(padded, dim, 2, (0, 1)) for dim in (0, 1)]
    spread = lower[0] + upper[0] + lower[1] + upper[1] - 4.0 * middle
    return middle + 0.1 * spread + 0.2 * middle * (1.0 - middle * crowding)


def reference(tracer, crowding):
    for step in range(STEPS):
        tracer = one_step(jnp.pad(tracer, ((1, 1), (1, 1), (0, 0)), mode="constant"), crowding)
    potential = jnp.cumsum(tracer, axis=1) / GRID_X
    return potential, tracer
```

```python
import functools

import jax
import jax.numpy as jnp
from jax import lax
from jax.experimental import pallas as pl
from jax.experimental.pallas import tpu as pltpu
from jax.sharding import PartitionSpec as P

STEPS = 6
MESH = pl.DeviceIdType.MESH
LANES = 8


def chunk_rows(height):
    for rows in (16, 24, 32, 8):
        if height % rows == 0:
            return rows
    return height


def kernel(
    sizes, t_hbm, c_hbm, pot_hbm, end_hbm,
    buf, crowd, pot, col_send, col_recv, row_send, row_recv,
    total, pair_recv, pair_sum, group_recv,
    load_t, load_c, store_pot, store_end,
    col_ssem, col_rsem, row_ssem, row_rsem,
    pair_ssem, pair_rsem, group_ssem, group_rsem,
):
    height, width, n_rows, n_cols = sizes
    rc = chunk_rows(height)
    chunks = height // rc
    inner = 2 if n_cols % 2 == 0 else 1
    groups = n_cols // inner
    unroll = 8
    row, col = lax.axis_index("rows"), lax.axis_index("cols")
    member, group = lax.rem(col, inner), lax.div(col, inner)
    zero8 = jnp.zeros((LANES, buf.shape[-1]), jnp.float32)

    def at_col(c):
        return {"rows": row, "cols": c}

    def at_row(r):
        return {"rows": r, "cols": col}

    loads = []
    for r in range(chunks):
        part = pl.ds(r * rc * width, rc * width)
        loads.append(pltpu.make_async_copy(
            t_hbm.at[part], buf.at[0, pl.ds((1 + r * rc) * width, rc * width)], load_t.at[r]))
    for load in loads:
        load.start()
    crowd_loads = []
    for r in range(chunks):
        part = pl.ds(r * rc * width, rc * width)
        crowd_loads.append(pltpu.make_async_copy(c_hbm.at[part], crowd.at[part], load_c.at[r]))
    for load in crowd_loads:
        load.start()

    barrier = pltpu.get_barrier_semaphore()

    def greet(there, device):
        @pl.when(there)
        def _():
            pl.semaphore_signal(barrier, inc=1, device_id=device, device_id_type=MESH)
        return there.astype(jnp.int32)

    has_left, has_right = col > 0, col < n_cols - 1
    has_up, has_down = row > 0, row < n_rows - 1
    met = greet(has_left, at_col(col - 1)) + greet(has_right, at_col(col + 1))
    met += greet(has_up, at_row(row - 1)) + greet(has_down, at_row(row + 1))
    for gap in range(1, groups):
        if gap * inner == 1:
            continue
        met += greet(group >= gap, at_col(col - gap * inner))
        met += greet(group + gap < groups, at_col(col + gap * inner))

    for side, there in ((0, has_left), (1, has_right)):
        @pl.when(jnp.logical_not(there))
        def _():
            @pl.loop(0, STEPS * height // LANES)
            def _(i):
                s, y = lax.div(i, height // LANES), lax.rem(i, height // LANES)
                col_recv[s, side, pl.ds(pl.multiple_of(y * LANES, LANES), LANES)] = zero8
    for side, there in ((0, has_up), (1, has_down)):
        @pl.when(jnp.logical_not(there))
        def _():
            @pl.loop(0, STEPS * width // LANES)
            def _(i):
                s, x = lax.div(i, width // LANES), lax.rem(i, width // LANES)
                row_recv[s, side, pl.ds(pl.multiple_of(x * LANES, LANES), LANES)] = zero8

    pl.semaphore_wait(barrier, met)

    def col_copy(s, side, r):
        rows = pl.ds(r * rc, rc)
        return pltpu.make_async_remote_copy(
            src_ref=col_send.at[s, side, rows], dst_ref=col_recv.at[s, 1 - side, rows],
            send_sem=col_ssem.at[s, side, r], recv_sem=col_rsem.at[s, 1 - side, r],
            device_id=at_col(col - 1 if side == 0 else col + 1), device_id_type=MESH)

    def col_arrival(s, side, r):
        rows = pl.ds(r * rc, rc)
        return pltpu.make_async_remote_copy(
            src_ref=col_send.at[s, side, rows], dst_ref=col_recv.at[s, side, rows],
            send_sem=col_ssem.at[s, side, r], recv_sem=col_rsem.at[s, side, r],
            device_id=at_col(col - 1 if side == 0 else col + 1), device_id_type=MESH)

    def row_copy(s, side):
        return pltpu.make_async_remote_copy(
            src_ref=row_send.at[s, side], dst_ref=row_recv.at[s, 1 - side],
            send_sem=row_ssem.at[s, side], recv_sem=row_rsem.at[s, 1 - side],
            device_id=at_row(row - 1 if side == 0 else row + 1), device_id_type=MESH)

    def row_arrival(s, side):
        return pltpu.make_async_remote_copy(
            src_ref=row_send.at[s, side], dst_ref=row_recv.at[s, side],
            send_sem=row_ssem.at[s, side], recv_sem=row_rsem.at[s, side],
            device_id=at_row(row - 1 if side == 0 else row + 1), device_id_type=MESH)

    def send_edges(p, s, r):
        for side, x in ((0, 0), (1, width - 1)):
            for y in range(r * rc, r * rc + rc, LANES):
                col_send[s, side, pl.ds(y, LANES)] = buf[p, pl.ds((1 + y) * width + x, LANES, stride=width)]
        for side, y, there in ((0, 0, has_up), (1, height - 1, has_down)):
            if r == y // rc:
                @pl.when(there)
                def _():
                    row_send[s, side] = buf[p, pl.ds((1 + y) * width, width)]
                    row_copy(s, side).start()
        for side, there in ((0, has_left), (1, has_right)):
            @pl.when(there)
            def _():
                col_copy(s, side, r).start()

    for r in range(chunks):
        loads[r].wait()
        send_edges(0, 0, r)
    for r in range(chunks):
        crowd_loads[r].wait()

        @pl.loop(0, rc * width // (LANES * 8))
        def _(i):
            at = pl.ds(pl.multiple_of(r * rc * width + i * LANES * 8, LANES * 8), LANES * 8)
            crowd[at] = crowd[at] * 0.2

    place = lax.broadcasted_iota(jnp.int32, (LANES, buf.shape[-1]), 0)
    tiles = width // LANES

    def compute(p, q, s, r):
        for side, y, at in ((0, 0, 0), (1, height - 1, height + 1)):
            if r == y // rc:
                @pl.when((has_up, has_down)[side])
                def _():
                    row_arrival(s, side).wait_recv()
                buf[p, pl.ds(at * width, width)] = row_recv[s, side]
        for side, there in ((0, has_left), (1, has_right)):
            @pl.when(there)
            def _():
                col_arrival(s, side, r).wait_recv()

        @pl.loop(0, rc // unroll)
        def _(i):
            y0 = r * rc + i * unroll
            for j in range(tiles):
                o = pl.multiple_of((1 + y0) * width + j * LANES, LANES)
                rows = [buf[p, pl.ds(o + (u - 1) * width, LANES)] for u in range(unroll + 2)]
                for u in range(unroll):
                    middle = rows[u + 1]
                    before = buf[p, pl.ds(o + u * width - 1, LANES)]
                    after = buf[p, pl.ds(o + u * width + 1, LANES)]
                    if j == 0:
                        edge = jnp.broadcast_to(col_recv[s, 0, pl.ds(y0 + u, 1)], before.shape)
                        before = jnp.where(place == 0, edge, before)
                    if j == tiles - 1:
                        edge = jnp.broadcast_to(col_recv[s, 1, pl.ds(y0 + u, 1)], before.shape)
                        after = jnp.where(place == LANES - 1, edge, after)
                    c = crowd[pl.ds(o + (u - 1) * width, LANES)]
                    around = (rows[u] + rows[u + 2]) + (before + after)
                    buf[q, pl.ds(o + u * width, LANES)] = 0.1 * around + middle * (0.8 - middle * c)

    @pl.loop(0, STEPS - 1)
    def _(s):
        p = lax.rem(s, 2)
        for r in range(chunks):
            compute(p, 1 - p, s, r)
            send_edges(1 - p, s + 1, r)

    p, q = (STEPS - 1) % 2, STEPS % 2
    pair_to = col + 1 - 2 * member

    def pair_copy(r):
        rows = pl.ds(r * rc, rc)
        return pltpu.make_async_remote_copy(
            src_ref=total.at[rows], dst_ref=pair_recv.at[rows],
            send_sem=pair_ssem.at[r], recv_sem=pair_rsem.at[r],
            device_id=at_col(pair_to), device_id_type=MESH)

    def group_copy(gap, r):
        rows = pl.ds(r * rc, rc)
        return pltpu.make_async_remote_copy(
            src_ref=pair_sum.at[rows], dst_ref=group_recv.at[gap, rows],
            send_sem=group_ssem.at[gap, r], recv_sem=group_rsem.at[gap, r],
            device_id=at_col(col + gap * inner), device_id_type=MESH)

    def end_copy(r):
        return pltpu.make_async_copy(
            buf.at[q, pl.ds((1 + r * rc) * width, rc * width)],
            end_hbm.at[pl.ds(r * rc * width, rc * width)], store_end.at[r])

    def pot_copy(r):
        part = pl.ds(r * rc * width, rc * width)
        return pltpu.make_async_copy(pot.at[part], pot_hbm.at[part], store_pot.at[r])

    for r in range(chunks):
        compute(p, q, STEPS - 1, r)
        end_copy(r).start()

        @pl.loop(0, rc // LANES)
        def _(i):
            y = pl.multiple_of(r * rc + i * LANES, LANES)
            so_far = zero8
            for x in range(width):
                so_far = so_far + buf[q, pl.ds((1 + y) * width + x, LANES, stride=width)]
                pot[pl.ds(y * width + x, LANES, stride=width)] = so_far
            total[pl.ds(y, LANES)] = so_far
        if inner == 2:
            pair_copy(r).start()

    for r in range(chunks):
        rows = pl.ds(r * rc, rc)
        if inner == 2:
            pair_copy(r).wait_recv()
            pair_sum[rows] = total[rows] + pair_recv[rows]
        else:
            pair_sum[rows] = total[rows]
        for gap in range(1, groups):
            @pl.when(group + gap < groups)
            def _():
                group_copy(gap, r).start()

    scale = 1.0 / (width * n_cols)
    for r in range(chunks):
        rows = pl.ds(r * rc, rc)
        if inner == 2:
            pair_copy(r).wait_send()
            total[rows] = pair_recv[rows] * member.astype(jnp.float32)
        else:
            total[rows] = jnp.zeros((rc, buf.shape[-1]), jnp.float32)
        for gap in range(1, groups):
            @pl.when(group >= gap)
            def _():
                group_copy(gap, r).wait_recv()
                total[rows] += group_recv[gap, rows]

        @pl.loop(0, rc // LANES)
        def _(i):
            y = pl.multiple_of(r * rc + i * LANES, LANES)
            below = total[pl.ds(y, LANES)]
            for x in range(width):
                at = pl.ds(y * width + x, LANES, stride=width)
                pot[at] = (pot[at] + below) * scale
        pot_copy(r).start()

    for r in range(chunks):
        end_copy(r).wait()
        pot_copy(r).wait()

    @pl.loop(0, STEPS)
    def _(s):
        for side, there in ((0, has_left), (1, has_right)):
            @pl.when(there)
            def _():
                for r in range(chunks):
                    col_copy(s, side, r).wait_send()
        for side, there in ((0, has_up), (1, has_down)):
            @pl.when(there)
            def _():
                row_copy(s, side).wait_send()
    for gap in range(1, groups):
        @pl.when(group + gap < groups)
        def _():
            for r in range(chunks):
                group_copy(gap, r).wait_send()


def body(tracer, crowding):
    height, width, members = tracer.shape
    n_rows, n_cols = lax.axis_size("rows"), lax.axis_size("cols")
    chunks = height // chunk_rows(height)
    groups = n_cols // 2 if n_cols % 2 == 0 else n_cols
    cells = height * width
    f32 = jnp.float32
    dma = pltpu.SemaphoreType.DMA
    out = jax.ShapeDtypeStruct((cells, members), f32)
    potential, end = pl.pallas_call(
        functools.partial(kernel, (height, width, n_rows, n_cols)),
        out_shape=(out, out),
        in_specs=[pl.BlockSpec(memory_space=pl.ANY)] * 2,
        out_specs=[pl.BlockSpec(memory_space=pl.ANY)] * 2,
        scratch_shapes=[
            pltpu.VMEM((2, (height + 2) * width, members), f32),
            pltpu.VMEM((cells, members), f32),
            pltpu.VMEM((cells, members), f32),
            pltpu.VMEM((STEPS, 2, height, members), f32),
            pltpu.VMEM((STEPS, 2, height, members), f32),
            pltpu.VMEM((STEPS, 2, width, members), f32),
            pltpu.VMEM((STEPS, 2, width, members), f32),
            pltpu.VMEM((height, members), f32),
            pltpu.VMEM((height, members), f32),
            pltpu.VMEM((height, members), f32),
            pltpu.VMEM((groups, height, members), f32),
            dma((chunks,)), dma((chunks,)), dma((chunks,)), dma((chunks,)),
            dma((STEPS, 2, chunks)), dma((STEPS, 2, chunks)),
            dma((STEPS, 2)), dma((STEPS, 2)),
            dma((chunks,)), dma((chunks,)),
            dma((groups, chunks)), dma((groups, chunks)),
        ],
        compiler_params=pltpu.CompilerParams(collective_id=0, has_side_effects=True),
    )(tracer.reshape(cells, members), crowding.reshape(cells, members))
    return potential.reshape(tracer.shape), end.reshape(tracer.shape)


def solution(mesh):
    return jax.shard_map(
        body,
        mesh=mesh,
        in_specs=(P("rows", "cols", None), P("rows", "cols", None)),
        out_specs=(P("rows", "cols", None), P("rows", "cols", None)),
        check_vma=False,
    )
```

```python
import functools

import jax
import jax.numpy as jnp
from jax import lax
from jax.experimental import pallas as pl
from jax.experimental.pallas import tpu as pltpu
from jax.sharding import PartitionSpec as P

STEPS = 6
MESH = pl.DeviceIdType.MESH
LANES = 8
GRANT = 24 * 2**20


def chunk_rows(height):
    for rows in (16, 24, 32, 8):
        if height % rows == 0:
            return rows
    return height


def kernel(
    sizes, t_hbm, c_hbm, end, here, below,
    buf, crowd, col_send, col_recv, row_send, row_recv,
    total, pair_recv, pair_sum, group_recv,
    load_t, load_c,
    col_ssem, col_rsem, row_ssem, row_rsem,
    pair_ssem, pair_rsem, group_ssem, group_rsem,
):
    height, width, n_rows, n_cols = sizes
    rc = chunk_rows(height)
    chunks = height // rc
    inner = 2 if n_cols % 2 == 0 else 1
    groups = n_cols // inner
    unroll = 8
    row, col = lax.axis_index("rows"), lax.axis_index("cols")
    member, group = lax.rem(col, inner), lax.div(col, inner)
    zero8 = jnp.zeros((LANES, buf.shape[-1]), jnp.float32)

    def at_col(c):
        return {"rows": row, "cols": c}

    def at_row(r):
        return {"rows": r, "cols": col}

    loads = []
    for r in range(chunks):
        part = pl.ds(r * rc * width, rc * width)
        loads.append(pltpu.make_async_copy(
            t_hbm.at[part], buf.at[0, pl.ds((1 + r * rc) * width, rc * width)], load_t.at[r]))
    for load in loads:
        load.start()
    crowd_loads = []
    for r in range(chunks):
        part = pl.ds(r * rc * width, rc * width)
        crowd_loads.append(pltpu.make_async_copy(c_hbm.at[part], crowd.at[part], load_c.at[r]))
    for load in crowd_loads:
        load.start()

    barrier = pltpu.get_barrier_semaphore()

    def greet(there, device):
        @pl.when(there)
        def _():
            pl.semaphore_signal(barrier, inc=1, device_id=device, device_id_type=MESH)
        return there.astype(jnp.int32)

    has_left, has_right = col > 0, col < n_cols - 1
    has_up, has_down = row > 0, row < n_rows - 1
    met = greet(has_left, at_col(col - 1)) + greet(has_right, at_col(col + 1))
    met += greet(has_up, at_row(row - 1)) + greet(has_down, at_row(row + 1))
    for gap in range(1, groups):
        if gap * inner == 1:
            continue
        met += greet(group >= gap, at_col(col - gap * inner))
        met += greet(group + gap < groups, at_col(col + gap * inner))

    for side, there in ((0, has_left), (1, has_right)):
        @pl.when(jnp.logical_not(there))
        def _():
            @pl.loop(0, STEPS * height // LANES)
            def _(i):
                s, y = lax.div(i, height // LANES), lax.rem(i, height // LANES)
                col_recv[s, side, pl.ds(pl.multiple_of(y * LANES, LANES), LANES)] = zero8
    for side, there in ((0, has_up), (1, has_down)):
        @pl.when(jnp.logical_not(there))
        def _():
            @pl.loop(0, STEPS * width // LANES)
            def _(i):
                s, x = lax.div(i, width // LANES), lax.rem(i, width // LANES)
                row_recv[s, side, pl.ds(pl.multiple_of(x * LANES, LANES), LANES)] = zero8

    pl.semaphore_wait(barrier, met)

    def col_copy(s, side, r):
        rows = pl.ds(r * rc, rc)
        return pltpu.make_async_remote_copy(
            src_ref=col_send.at[s, side, rows], dst_ref=col_recv.at[s, 1 - side, rows],
            send_sem=col_ssem.at[s, side, r], recv_sem=col_rsem.at[s, 1 - side, r],
            device_id=at_col(col - 1 if side == 0 else col + 1), device_id_type=MESH)

    def col_arrival(s, side, r):
        rows = pl.ds(r * rc, rc)
        return pltpu.make_async_remote_copy(
            src_ref=col_send.at[s, side, rows], dst_ref=col_recv.at[s, side, rows],
            send_sem=col_ssem.at[s, side, r], recv_sem=col_rsem.at[s, side, r],
            device_id=at_col(col - 1 if side == 0 else col + 1), device_id_type=MESH)

    def row_copy(s, side):
        return pltpu.make_async_remote_copy(
            src_ref=row_send.at[s, side], dst_ref=row_recv.at[s, 1 - side],
            send_sem=row_ssem.at[s, side], recv_sem=row_rsem.at[s, 1 - side],
            device_id=at_row(row - 1 if side == 0 else row + 1), device_id_type=MESH)

    def row_arrival(s, side):
        return pltpu.make_async_remote_copy(
            src_ref=row_send.at[s, side], dst_ref=row_recv.at[s, side],
            send_sem=row_ssem.at[s, side], recv_sem=row_rsem.at[s, side],
            device_id=at_row(row - 1 if side == 0 else row + 1), device_id_type=MESH)

    def send_edges(p, s, r):
        for side, x in ((0, 0), (1, width - 1)):
            for y in range(r * rc, r * rc + rc, LANES):
                col_send[s, side, pl.ds(y, LANES)] = buf[p, pl.ds((1 + y) * width + x, LANES, stride=width)]
        for side, y, there in ((0, 0, has_up), (1, height - 1, has_down)):
            if r == y // rc:
                @pl.when(there)
                def _():
                    row_send[s, side] = buf[p, pl.ds((1 + y) * width, width)]
                    row_copy(s, side).start()
        for side, there in ((0, has_left), (1, has_right)):
            @pl.when(there)
            def _():
                col_copy(s, side, r).start()

    for r in range(chunks):
        loads[r].wait()
        send_edges(0, 0, r)
    for r in range(chunks):
        crowd_loads[r].wait()

        @pl.loop(0, rc * width // (LANES * 8))
        def _(i):
            at = pl.ds(pl.multiple_of(r * rc * width + i * LANES * 8, LANES * 8), LANES * 8)
            crowd[at] = crowd[at] * 0.2

    place = lax.broadcasted_iota(jnp.int32, (LANES, buf.shape[-1]), 0)
    tiles = width // LANES

    def compute(p, q, s, r, last=False):
        for side, y, at in ((0, 0, 0), (1, height - 1, height + 1)):
            if r == y // rc:
                @pl.when((has_up, has_down)[side])
                def _():
                    row_arrival(s, side).wait_recv()
                buf[p, pl.ds(at * width, width)] = row_recv[s, side]
        for side, there in ((0, has_left), (1, has_right)):
            @pl.when(there)
            def _():
                col_arrival(s, side, r).wait_recv()

        @pl.loop(0, rc // unroll)
        def _(i):
            y0 = r * rc + i * unroll
            base = pl.multiple_of((1 + y0) * width, LANES)

            def line(u):
                return [buf[p, pl.ds(base + u * width + j * LANES, LANES)] for j in range(tiles)]

            above, middle = line(-1), line(0)
            for u in range(unroll):
                under = line(u + 1)
                forth = [pltpu.roll(m, 1, 0) for m in middle]
                back = [pltpu.roll(m, LANES - 1, 0) for m in middle]
                first = jnp.broadcast_to(col_recv[s, 0, pl.ds(y0 + u, 1)], zero8.shape)
                final = jnp.broadcast_to(col_recv[s, 1, pl.ds(y0 + u, 1)], zero8.shape)
                news = []
                for j in range(tiles):
                    before = jnp.where(place == 0, forth[j - 1] if j else first, forth[j])
                    after = jnp.where(place == LANES - 1, back[j + 1] if j + 1 < tiles else final, back[j])
                    c = crowd[pl.ds(base + (u - 1) * width + j * LANES, LANES)]
                    around = (above[j] + under[j]) + (before + after)
                    new = 0.1 * around + middle[j] * (0.8 - middle[j] * c)
                    news.append(new)
                    if last:
                        end[pl.ds(base + (u - 1) * width + j * LANES, LANES)] = new
                    else:
                        buf[q, pl.ds(base + u * width + j * LANES, LANES)] = new
                if last:
                    whole = functools.reduce(jnp.add, news)
                    total[pl.ds(y0 + u, 1)] = jnp.sum(whole, axis=0, keepdims=True)
                above, middle = middle, under

    @pl.loop(0, STEPS - 1)
    def _(s):
        p = lax.rem(s, 2)
        for r in range(chunks):
            compute(p, 1 - p, s, r)
            send_edges(1 - p, s + 1, r)

    p, q = (STEPS - 1) % 2, STEPS % 2
    pair_to = col + 1 - 2 * member

    def pair_copy(r):
        rows = pl.ds(r * rc, rc)
        return pltpu.make_async_remote_copy(
            src_ref=total.at[rows], dst_ref=pair_recv.at[rows],
            send_sem=pair_ssem.at[r], recv_sem=pair_rsem.at[r],
            device_id=at_col(pair_to), device_id_type=MESH)

    def group_copy(gap, r):
        rows = pl.ds(r * rc, rc)
        return pltpu.make_async_remote_copy(
            src_ref=pair_sum.at[rows], dst_ref=group_recv.at[gap, rows],
            send_sem=group_ssem.at[gap, r], recv_sem=group_rsem.at[gap, r],
            device_id=at_col(col + gap * inner), device_id_type=MESH)

    def sum_along(r):
        @pl.loop(0, rc // LANES)
        def _(i):
            y = pl.multiple_of(r * rc + i * LANES, LANES)
            so_far = zero8
            for x in range(width):
                at = pl.ds(y * width + x, LANES, stride=width)
                so_far = so_far + end[at]
                here[at] = so_far

    for r in range(chunks):
        compute(p, q, STEPS - 1, r, last=True)
        if inner == 2:
            pair_copy(r).start()

    early = chunks // 2
    for r in range(early):
        sum_along(r)

    for r in range(chunks):
        rows = pl.ds(r * rc, rc)
        if inner == 2:
            pair_copy(r).wait_recv()
            pair_sum[rows] = total[rows] + pair_recv[rows]
        else:
            pair_sum[rows] = total[rows]
        for gap in range(1, groups):
            @pl.when(group + gap < groups)
            def _():
                group_copy(gap, r).start()

    for r in range(early, chunks):
        sum_along(r)

    for r in range(chunks):
        rows = pl.ds(r * rc, rc)
        if inner == 2:
            pair_copy(r).wait_send()
            below[rows] = pair_recv[rows] * member.astype(jnp.float32)
        else:
            below[rows] = jnp.zeros((rc, buf.shape[-1]), jnp.float32)
        for gap in range(1, groups):
            @pl.when(group >= gap)
            def _():
                group_copy(gap, r).wait_recv()
                below[rows] += group_recv[gap, rows]

    @pl.loop(0, STEPS)
    def _(s):
        for side, there in ((0, has_left), (1, has_right)):
            @pl.when(there)
            def _():
                for r in range(chunks):
                    col_copy(s, side, r).wait_send()
        for side, there in ((0, has_up), (1, has_down)):
            @pl.when(there)
            def _():
                row_copy(s, side).wait_send()
    for gap in range(1, groups):
        @pl.when(group + gap < groups)
        def _():
            for r in range(chunks):
                group_copy(gap, r).wait_send()


def finish(sizes, end, here, below, pot_hbm, end_hbm, pot, pot_sem, end_sem):
    height, width, n_cols = sizes
    rc = chunk_rows(height)
    end_copy = pltpu.make_async_copy(end, end_hbm, end_sem)
    end_copy.start()
    scale = 1.0 / (width * n_cols)

    def pot_copy(r):
        part = pl.ds(r * rc * width, rc * width)
        return pltpu.make_async_copy(pot.at[part], pot_hbm.at[part], pot_sem.at[r])

    for r in range(height // rc):
        @pl.loop(0, rc // LANES)
        def _(i):
            for u in range(LANES):
                y = r * rc + i * LANES + u
                earlier = jnp.broadcast_to(below[pl.ds(y, 1)], (LANES, pot.shape[-1]))
                for x in range(0, width, LANES):
                    at = pl.ds(pl.multiple_of(y * width + x, LANES), LANES)
                    pot[at] = (here[at] + earlier) * scale
        pot_copy(r).start()
    end_copy.wait()
    for r in range(height // rc):
        pot_copy(r).wait()


def body(tracer, crowding):
    height, width, members = tracer.shape
    n_rows, n_cols = lax.axis_size("rows"), lax.axis_size("cols")
    chunks = height // chunk_rows(height)
    groups = n_cols // 2 if n_cols % 2 == 0 else n_cols
    cells = height * width
    f32 = jnp.float32
    dma = pltpu.SemaphoreType.DMA
    out = jax.ShapeDtypeStruct((cells, members), f32)
    end, here, below = pl.pallas_call(
        functools.partial(kernel, (height, width, n_rows, n_cols)),
        out_shape=(
            pltpu.VMEM((cells, members), f32),
            pltpu.VMEM((cells, members), f32),
            pltpu.VMEM((height, members), f32),
        ),
        in_specs=[pl.BlockSpec(memory_space=pltpu.HBM)] * 2,
        out_specs=[pl.BlockSpec(memory_space=pltpu.VMEM)] * 3,
        scratch_shapes=[
            pltpu.VMEM((2, (height + 2) * width, members), f32),
            pltpu.VMEM((cells, members), f32),
            pltpu.VMEM((STEPS, 2, height, members), f32),
            pltpu.VMEM((STEPS, 2, height, members), f32),
            pltpu.VMEM((STEPS, 2, width, members), f32),
            pltpu.VMEM((STEPS, 2, width, members), f32),
            pltpu.VMEM((height, members), f32),
            pltpu.VMEM((height, members), f32),
            pltpu.VMEM((height, members), f32),
            pltpu.VMEM((groups, height, members), f32),
            dma((chunks,)), dma((chunks,)),
            dma((STEPS, 2, chunks)), dma((STEPS, 2, chunks)),
            dma((STEPS, 2)), dma((STEPS, 2)),
            dma((chunks,)), dma((chunks,)),
            dma((groups, chunks)), dma((groups, chunks)),
        ],
        compiler_params=pltpu.CompilerParams(
            collective_id=0, has_side_effects=True, vmem_limit_bytes=GRANT),
    )(tracer.reshape(cells, members), crowding.reshape(cells, members))
    potential, end = pl.pallas_call(
        functools.partial(finish, (height, width, n_cols)),
        out_shape=(out, out),
        in_specs=[pl.BlockSpec(memory_space=pltpu.VMEM)] * 3,
        out_specs=[pl.BlockSpec(memory_space=pl.ANY)] * 2,
        scratch_shapes=[pltpu.VMEM((cells, members), f32), dma((chunks,)), dma],
        compiler_params=pltpu.CompilerParams(vmem_limit_bytes=GRANT),
    )(end, here, below)
    return potential.reshape(tracer.shape), end.reshape(tracer.shape)


def solution(mesh):
    return jax.shard_map(
        body,
        mesh=mesh,
        in_specs=(P("rows", "cols", None), P("rows", "cols", None)),
        out_specs=(P("rows", "cols", None), P("rows", "cols", None)),
        check_vma=False,
    )
```

```python
import functools

import jax
import jax.numpy as jnp
from jax import lax
from jax.experimental import pallas as pl
from jax.experimental.pallas import tpu as pltpu
from jax.sharding import PartitionSpec as P

STEPS = 6
MESH = pl.DeviceIdType.MESH
LANES = 8
GRANT = 24 * 2**20


def chunk_rows(height):
    for rows in (16, 24, 32, 8):
        if height % rows == 0:
            return rows
    return height


def kernel(
    sizes, t_hbm, c_hbm, end, here, below,
    buf, crowd, col_send, col_recv, row_send, row_recv,
    total, pair_recv, pair_sum, group_recv,
    load_t, load_c,
    col_ssem, col_rsem, row_ssem, row_rsem,
    pair_ssem, pair_rsem, group_ssem, group_rsem,
):
    height, width, n_rows, n_cols = sizes
    rc = chunk_rows(height)
    chunks = height // rc
    inner = 2 if n_cols % 2 == 0 else 1
    groups = n_cols // inner
    unroll = 8
    row, col = lax.axis_index("rows"), lax.axis_index("cols")
    member, group = lax.rem(col, inner), lax.div(col, inner)
    zero8 = jnp.zeros((LANES, buf.shape[-1]), jnp.float32)

    def at_col(c):
        return {"rows": row, "cols": c}

    def at_row(r):
        return {"rows": r, "cols": col}

    loads = []
    for r in range(chunks):
        part = pl.ds(r * rc * width, rc * width)
        loads.append(pltpu.make_async_copy(
            t_hbm.at[part], buf.at[0, pl.ds((1 + r * rc) * width, rc * width)], load_t.at[r]))
    for load in loads:
        load.start()
    crowd_loads = []
    for r in range(chunks):
        part = pl.ds(r * rc * width, rc * width)
        crowd_loads.append(pltpu.make_async_copy(c_hbm.at[part], crowd.at[part], load_c.at[r]))
    for load in crowd_loads:
        load.start()

    barrier = pltpu.get_barrier_semaphore()

    def greet(there, device):
        @pl.when(there)
        def _():
            pl.semaphore_signal(barrier, inc=1, device_id=device, device_id_type=MESH)
        return there.astype(jnp.int32)

    has_left, has_right = col > 0, col < n_cols - 1
    has_up, has_down = row > 0, row < n_rows - 1
    met = greet(has_left, at_col(col - 1)) + greet(has_right, at_col(col + 1))
    met += greet(has_up, at_row(row - 1)) + greet(has_down, at_row(row + 1))
    for gap in range(1, groups):
        if gap * inner == 1:
            continue
        met += greet(group >= gap, at_col(col - gap * inner))
        met += greet(group + gap < groups, at_col(col + gap * inner))

    for side, there in ((0, has_left), (1, has_right)):
        @pl.when(jnp.logical_not(there))
        def _():
            @pl.loop(0, STEPS * height // LANES)
            def _(i):
                s, y = lax.div(i, height // LANES), lax.rem(i, height // LANES)
                col_recv[s, side, pl.ds(pl.multiple_of(y * LANES, LANES), LANES)] = zero8
    for side, there in ((0, has_up), (1, has_down)):
        @pl.when(jnp.logical_not(there))
        def _():
            @pl.loop(0, STEPS * width // LANES)
            def _(i):
                s, x = lax.div(i, width // LANES), lax.rem(i, width // LANES)
                row_recv[s, side, pl.ds(pl.multiple_of(x * LANES, LANES), LANES)] = zero8

    pl.semaphore_wait(barrier, met)

    def col_copy(s, side, r):
        rows = pl.ds(r * rc, rc)
        return pltpu.make_async_remote_copy(
            src_ref=col_send.at[s, side, rows], dst_ref=col_recv.at[s, 1 - side, rows],
            send_sem=col_ssem.at[s, side, r], recv_sem=col_rsem.at[s, 1 - side, r],
            device_id=at_col(col - 1 if side == 0 else col + 1), device_id_type=MESH)

    def col_arrival(s, side, r):
        rows = pl.ds(r * rc, rc)
        return pltpu.make_async_remote_copy(
            src_ref=col_send.at[s, side, rows], dst_ref=col_recv.at[s, side, rows],
            send_sem=col_ssem.at[s, side, r], recv_sem=col_rsem.at[s, side, r],
            device_id=at_col(col - 1 if side == 0 else col + 1), device_id_type=MESH)

    def row_copy(s, side):
        return pltpu.make_async_remote_copy(
            src_ref=row_send.at[s, side], dst_ref=row_recv.at[s, 1 - side],
            send_sem=row_ssem.at[s, side], recv_sem=row_rsem.at[s, 1 - side],
            device_id=at_row(row - 1 if side == 0 else row + 1), device_id_type=MESH)

    def row_arrival(s, side):
        return pltpu.make_async_remote_copy(
            src_ref=row_send.at[s, side], dst_ref=row_recv.at[s, side],
            send_sem=row_ssem.at[s, side], recv_sem=row_rsem.at[s, side],
            device_id=at_row(row - 1 if side == 0 else row + 1), device_id_type=MESH)

    def send_edges(p, s, r):
        for side, x in ((0, 0), (1, width - 1)):
            for y in range(r * rc, r * rc + rc, LANES):
                col_send[s, side, pl.ds(y, LANES)] = buf[p, pl.ds((1 + y) * width + x, LANES, stride=width)]
        for side, y, there in ((0, 0, has_up), (1, height - 1, has_down)):
            if r == y // rc:
                @pl.when(there)
                def _():
                    row_send[s, side] = buf[p, pl.ds((1 + y) * width, width)]
                    row_copy(s, side).start()
        odd = lax.rem(col, 2) == 1
        for side, there in ((0, has_left & jnp.logical_not(odd)), (1, has_right), (0, has_left & odd)):
            @pl.when(there)
            def _():
                col_copy(s, side, r).start()

    for r in range(chunks):
        loads[r].wait()
        send_edges(0, 0, r)
    for r in range(chunks):
        crowd_loads[r].wait()

        @pl.loop(0, rc * width // (LANES * 8))
        def _(i):
            at = pl.ds(pl.multiple_of(r * rc * width + i * LANES * 8, LANES * 8), LANES * 8)
            crowd[at] = crowd[at] * 0.2

    place = lax.broadcasted_iota(jnp.int32, (LANES, buf.shape[-1]), 0)
    tiles = width // LANES

    def compute(p, q, s, r, last=False):
        for side, y, at in ((0, 0, 0), (1, height - 1, height + 1)):
            if r == y // rc:
                @pl.when((has_up, has_down)[side])
                def _():
                    row_arrival(s, side).wait_recv()
                buf[p, pl.ds(at * width, width)] = row_recv[s, side]
        for side, there in ((0, has_left), (1, has_right)):
            @pl.when(there)
            def _():
                col_arrival(s, side, r).wait_recv()

        @pl.loop(0, rc // unroll)
        def _(i):
            y0 = r * rc + i * unroll
            base = pl.multiple_of((1 + y0) * width, LANES)

            def line(u):
                return [buf[p, pl.ds(base + u * width + j * LANES, LANES)] for j in range(tiles)]

            above, middle = line(-1), line(0)
            for u in range(unroll):
                under = line(u + 1)
                forth = [pltpu.roll(m, 1, 0) for m in middle]
                back = [pltpu.roll(m, LANES - 1, 0) for m in middle]
                first = jnp.broadcast_to(col_recv[s, 0, pl.ds(y0 + u, 1)], zero8.shape)
                final = jnp.broadcast_to(col_recv[s, 1, pl.ds(y0 + u, 1)], zero8.shape)
                news = []
                for j in range(tiles):
                    before = jnp.where(place == 0, forth[j - 1] if j else first, forth[j])
                    after = jnp.where(place == LANES - 1, back[j + 1] if j + 1 < tiles else final, back[j])
                    c = crowd[pl.ds(base + (u - 1) * width + j * LANES, LANES)]
                    around = (above[j] + under[j]) + (before + after)
                    new = 0.1 * around + middle[j] * (0.8 - middle[j] * c)
                    news.append(new)
                    if last:
                        end[pl.ds(base + (u - 1) * width + j * LANES, LANES)] = new
                    else:
                        buf[q, pl.ds(base + u * width + j * LANES, LANES)] = new
                if last:
                    whole = functools.reduce(jnp.add, news)
                    total[pl.ds(y0 + u, 1)] = jnp.sum(whole, axis=0, keepdims=True)
                above, middle = middle, under

    @pl.loop(0, STEPS - 1)
    def _(s):
        p = lax.rem(s, 2)
        for r in range(chunks):
            compute(p, 1 - p, s, r)
            send_edges(1 - p, s + 1, r)

    p, q = (STEPS - 1) % 2, STEPS % 2
    pair_to = col + 1 - 2 * member

    def pair_copy(r):
        rows = pl.ds(r * rc, rc)
        return pltpu.make_async_remote_copy(
            src_ref=total.at[rows], dst_ref=pair_recv.at[rows],
            send_sem=pair_ssem.at[r], recv_sem=pair_rsem.at[r],
            device_id=at_col(pair_to), device_id_type=MESH)

    def group_copy(gap, r):
        rows = pl.ds(r * rc, rc)
        return pltpu.make_async_remote_copy(
            src_ref=pair_sum.at[rows], dst_ref=group_recv.at[gap, rows],
            send_sem=group_ssem.at[gap, r], recv_sem=group_rsem.at[gap, r],
            device_id=at_col(col + gap * inner), device_id_type=MESH)

    def sum_along(r):
        @pl.loop(0, rc // LANES)
        def _(i):
            y = pl.multiple_of(r * rc + i * LANES, LANES)
            so_far = zero8
            for x in range(width):
                at = pl.ds(y * width + x, LANES, stride=width)
                so_far = so_far + end[at]
                here[at] = so_far

    for r in range(chunks):
        compute(p, q, STEPS - 1, r, last=True)
        if inner == 2:
            pair_copy(r).start()

    early = chunks // 2
    for r in range(early):
        sum_along(r)

    for r in range(chunks):
        rows = pl.ds(r * rc, rc)
        if inner == 2:
            pair_copy(r).wait_recv()
            pair_sum[rows] = total[rows] + pair_recv[rows]
        else:
            pair_sum[rows] = total[rows]
        for gap in range(groups - 1, 0, -1):
            @pl.when(group + gap < groups)
            def _():
                group_copy(gap, r).start()

    for r in range(early, chunks):
        sum_along(r)

    for r in range(chunks):
        rows = pl.ds(r * rc, rc)
        if inner == 2:
            pair_copy(r).wait_send()
            below[rows] = pair_recv[rows] * member.astype(jnp.float32)
        else:
            below[rows] = jnp.zeros((rc, buf.shape[-1]), jnp.float32)
        for gap in range(1, groups):
            @pl.when(group >= gap)
            def _():
                group_copy(gap, r).wait_recv()
                below[rows] += group_recv[gap, rows]

    @pl.loop(0, STEPS)
    def _(s):
        for side, there in ((0, has_left), (1, has_right)):
            @pl.when(there)
            def _():
                for r in range(chunks):
                    col_copy(s, side, r).wait_send()
        for side, there in ((0, has_up), (1, has_down)):
            @pl.when(there)
            def _():
                row_copy(s, side).wait_send()
    for gap in range(1, groups):
        @pl.when(group + gap < groups)
        def _():
            for r in range(chunks):
                group_copy(gap, r).wait_send()


def finish(sizes, end, here, below, pot_hbm, end_hbm, pot, pot_sem, end_sem):
    height, width, n_cols = sizes
    rc = chunk_rows(height)
    end_copy = pltpu.make_async_copy(end, end_hbm, end_sem)
    end_copy.start()
    scale = 1.0 / (width * n_cols)

    def pot_copy(r):
        part = pl.ds(r * rc * width, rc * width)
        return pltpu.make_async_copy(pot.at[part], pot_hbm.at[part], pot_sem.at[r])

    for r in range(height // rc):
        @pl.loop(0, rc // LANES)
        def _(i):
            for u in range(LANES):
                y = r * rc + i * LANES + u
                earlier = jnp.broadcast_to(below[pl.ds(y, 1)], (LANES, pot.shape[-1]))
                for x in range(0, width, LANES):
                    at = pl.ds(pl.multiple_of(y * width + x, LANES), LANES)
                    pot[at] = (here[at] + earlier) * scale
        pot_copy(r).start()
    end_copy.wait()
    for r in range(height // rc):
        pot_copy(r).wait()


def body(tracer, crowding):
    height, width, members = tracer.shape
    n_rows, n_cols = lax.axis_size("rows"), lax.axis_size("cols")
    chunks = height // chunk_rows(height)
    groups = n_cols // 2 if n_cols % 2 == 0 else n_cols
    cells = height * width
    f32 = jnp.float32
    dma = pltpu.SemaphoreType.DMA
    out = jax.ShapeDtypeStruct((cells, members), f32)
    end, here, below = pl.pallas_call(
        functools.partial(kernel, (height, width, n_rows, n_cols)),
        out_shape=(
            pltpu.VMEM((cells, members), f32),
            pltpu.VMEM((cells, members), f32),
            pltpu.VMEM((height, members), f32),
        ),
        in_specs=[pl.BlockSpec(memory_space=pltpu.HBM)] * 2,
        out_specs=[pl.BlockSpec(memory_space=pltpu.VMEM)] * 3,
        scratch_shapes=[
            pltpu.VMEM((2, (height + 2) * width, members), f32),
            pltpu.VMEM((cells, members), f32),
            pltpu.VMEM((STEPS, 2, height, members), f32),
            pltpu.VMEM((STEPS, 2, height, members), f32),
            pltpu.VMEM((STEPS, 2, width, members), f32),
            pltpu.VMEM((STEPS, 2, width, members), f32),
            pltpu.VMEM((height, members), f32),
            pltpu.VMEM((height, members), f32),
            pltpu.VMEM((height, members), f32),
            pltpu.VMEM((groups, height, members), f32),
            dma((chunks,)), dma((chunks,)),
            dma((STEPS, 2, chunks)), dma((STEPS, 2, chunks)),
            dma((STEPS, 2)), dma((STEPS, 2)),
            dma((chunks,)), dma((chunks,)),
            dma((groups, chunks)), dma((groups, chunks)),
        ],
        compiler_params=pltpu.CompilerParams(
            collective_id=0, has_side_effects=True, vmem_limit_bytes=GRANT),
    )(tracer.reshape(cells, members), crowding.reshape(cells, members))
    potential, end = pl.pallas_call(
        functools.partial(finish, (height, width, n_cols)),
        out_shape=(out, out),
        in_specs=[pl.BlockSpec(memory_space=pltpu.VMEM)] * 3,
        out_specs=[pl.BlockSpec(memory_space=pl.ANY)] * 2,
        scratch_shapes=[pltpu.VMEM((cells, members), f32), dma((chunks,)), dma],
        compiler_params=pltpu.CompilerParams(vmem_limit_bytes=GRANT),
    )(end, here, below)
    return potential.reshape(tracer.shape), end.reshape(tracer.shape)


def solution(mesh):
    return jax.shard_map(
        body,
        mesh=mesh,
        in_specs=(P("rows", "cols", None), P("rows", "cols", None)),
        out_specs=(P("rows", "cols", None), P("rows", "cols", None)),
        check_vma=False,
    )
```
